32 devices in a mesh: hot: 4 (over z), cold: 8 (over y, x, core).
Axes of the slice: x: 2, y: 2, z: 4, core: 2. Of those that a mesh axis runs over, the one named last changes fastest.
Arguments:
- tokens: bfloat16 [128, 8192], P('cold', 'hot'), may hold values from -6 to 6
- hot_gate: bfloat16 [8192, 1024], P('hot', 'cold'), may hold values from -0.0625 to 0.0625
- hot_up: bfloat16 [8192, 1024], P('hot', 'cold'), may hold values from -0.0625 to 0.0625
- hot_down: bfloat16 [1024, 8192], P('cold', 'hot'), may hold values from -0.125 to 0.125
- cold_gate: bfloat16 [8192, 6144], P('hot', 'cold'), may hold values from -0.0625 to 0.0625
- cold_up: bfloat16 [8192, 6144], P('hot', 'cold'), may hold values from -0.0625 to 0.0625
- cold_down: bfloat16 [6144, 8192], P('cold', 'hot'), may hold values from -0.125 to 0.125
- hot_ids: int32 [8], replicated, may hold values from 0 to 55, as said below
- cold_ids: int32 [48], replicated, may hold values from 0 to 55, as said below
- block_mask: int32 [128, 56], replicated, may hold values from 0 to 1, as said below
Outputs:
- mixed: bfloat16 [128, 8192], P('cold', 'hot')
The draws below stay inside these ranges and needn't reach their ends.
Inputs may be any that keep to these rules, and one draw needn't show every extreme that they name: hot_ids and cold_ids together name every block number from 0 to 55 once. `cold_ids`: cold slot s lies with index s // 6 of cold. `block_mask`: among the 16 tokens of one index of cold, at most 8 have a 1 in a cold slot of one given index of cold; in every draw some index of cold gets exactly 8 such tokens from every index of cold.
All inputs are finite; a program needn't handle non-finite values.
Results may differ from the reference program's by a relative error of at most 0.0049.
Values may be sent and summed in bfloat16 or wider, within the bound.
No kernel may reach another device: no remote copies, remote signals or barrier semaphores. Data moves between devices by JAX's collectives and lax.ppermute only.
A program may use at most 64 MiB of HBM per device.

```python
import jax
import jax.numpy as jnp
from jax import lax

D = 8192
BLOCK = 128
COLD_DEV = 6
TOK_DEV = 16
CAP = 8
TOKENS = 128
HB = 8
CB = 48
NB = 56
FF = 7168
N_COLD = 8


def rank_tokens(rank_key):
    return jax.random.permutation(rank_key, TOK_DEV).astype(jnp.int32)


def routing_tables(key):
    folded = jax.random.fold_in(key, 41)
    subkeys = jax.random.split(folded, 11)
    middle = (jax.random.permutation(subkeys[0], NB - 2) + 1).astype(jnp.int32)
    hot_list = jnp.concatenate([middle[:HB - 1], jnp.zeros((1,), jnp.int32)])
    cold_list = jnp.concatenate([middle[HB - 1:], jnp.full((1,), NB - 1, jnp.int32)])
    hot_ids = jnp.take(hot_list, jax.random.permutation(subkeys[9], HB).astype(jnp.int32))
    cold_ids = jnp.take(cold_list, jax.random.permutation(subkeys[10], CB).astype(jnp.int32))
    group_total = CB // COLD_DEV
    sources = TOKENS // TOK_DEV
    group_level = jax.random.randint(subkeys[1], (group_total,), 1, 5)
    busy_group = jax.random.randint(subkeys[2], (), 0, group_total)
    ceiling = group_level * CAP // 4
    hit_count = jax.random.randint(subkeys[3], (sources, group_total), 0, ceiling[None, :] + 1)
    hit_count = jnp.where(jnp.arange(group_total)[None, :] == busy_group, CAP, hit_count)
    rank_keys = jax.random.split(subkeys[4], sources * group_total)
    token_ranks = jax.vmap(rank_tokens)(rank_keys).reshape(sources, group_total, TOK_DEV)
    group_hit = token_ranks < hit_count[:, :, None]
    first_block = jax.random.randint(subkeys[5], (sources, group_total, TOK_DEV), 0, COLD_DEV)
    extra_blocks = jax.random.randint(subkeys[6], (sources, group_total, TOK_DEV, COLD_DEV), 0, 4) == 0
    chosen_blocks = (first_block[..., None] == jnp.arange(COLD_DEV)) | extra_blocks
    chosen_blocks = chosen_blocks & group_hit[..., None]
    cold_mask = jnp.transpose(chosen_blocks, (0, 2, 1, 3)).reshape(TOKENS, CB).astype(jnp.int32)
    hot_rate = jax.random.randint(subkeys[7], (HB,), 5, 10)
    hot_mask = (jax.random.randint(subkeys[8], (TOKENS, HB), 0, 10) < hot_rate[None, :]).astype(jnp.int32)
    block_mask = jnp.zeros((TOKENS, NB), jnp.int32)
    block_mask = block_mask.at[:, hot_ids].set(hot_mask)
    block_mask = block_mask.at[:, cold_ids].set(cold_mask)
    return (hot_ids, cold_ids, block_mask)


def draw_hot_ids(key, part):
    return routing_tables(key)[0]


def draw_cold_ids(key, part):
    return routing_tables(key)[1]


def draw_block_mask(key, part):
    return routing_tables(key)[2]


def steps_of(stream_key, dims, shards, low, high):
    gain, own = 1.0, jax.random.fold_in(stream_key, 6)
    for axis_at, parts in shards:
        heights = jnp.exp(jax.random.uniform(jax.random.fold_in(own, axis_at), (parts,), jnp.float32, low / len(shards), high / len(shards)))
        gain = gain * jnp.repeat(heights, dims[axis_at] // parts).reshape([-1 if axis == axis_at else 1 for axis in range(len(dims))])
    return gain


def scatter_about(own_key, shape, spread, bound, pieces=(), kind=jnp.bfloat16):
    result = spread * jax.random.normal(own_key, shape, jnp.float32)
    if pieces:
        result = result * steps_of(own_key, shape, pieces, -0.22, 0.18)
    return jnp.clip(result, -bound, bound).astype(kind)


def setup_inputs(seed: int = 0) -> dict:
    arg_keys = jax.random.split(jax.random.key(seed), 11)
    tokens = scatter_about(arg_keys[0], (TOKENS, D), 1.0, 6.0, ((0, 8), (1, 4)))
    hot_gate = scatter_about(arg_keys[1], (D, HB * BLOCK), D ** -0.5, 0.0625, ((0, 4), (1, 8)))
    hot_up = scatter_about(arg_keys[2], (D, HB * BLOCK), D ** -0.5, 0.0625, ((0, 4), (1, 8)))
    hot_down = scatter_about(arg_keys[3], (HB * BLOCK, D), (FF // 4) ** -0.5, 0.125, ((0, 8), (1, 4)))
    cold_gate = scatter_about(arg_keys[4], (D, CB * BLOCK), D ** -0.5, 0.0625, ((0, 4), (1, 8)))
    cold_up = scatter_about(arg_keys[5], (D, CB * BLOCK), D ** -0.5, 0.0625, ((0, 4), (1, 8)))
    cold_down = scatter_about(arg_keys[6], (CB * BLOCK, D), (FF // 4) ** -0.5, 0.125, ((0, 8), (1, 4)))
    hot_ids = draw_hot_ids(jax.random.fold_in(arg_keys[10], 71), 0)
    cold_ids = draw_cold_ids(jax.random.fold_in(arg_keys[10], 71), 0)
    block_mask = draw_block_mask(jax.random.fold_in(arg_keys[10], 71), 0)
    return dict(tokens=tokens, hot_gate=hot_gate, hot_up=hot_up, hot_down=hot_down, cold_gate=cold_gate, cold_up=cold_up, cold_down=cold_down, hot_ids=hot_ids, cold_ids=cold_ids, block_mask=block_mask)


def ranged_product(matrix_rows, weight):
    return jnp.dot(matrix_rows, weight, preferred_element_type=jnp.float32)


def reference(tokens, hot_gate, hot_up, hot_down, cold_gate, cold_up, cold_down, hot_ids, cold_ids, block_mask):
    hot_bits = jnp.take(block_mask, hot_ids, axis=1)
    cold_bits = jnp.take(block_mask, cold_ids, axis=1)
    hot_gates = ranged_product(tokens, hot_gate)
    hot_ups = ranged_product(tokens, hot_up)
    hot_scale = jnp.repeat(hot_bits.astype(jnp.float32), BLOCK, axis=1)
    hot_hidden = (jax.nn.silu(hot_gates) * hot_ups * hot_scale).astype(jnp.bfloat16)
    hot_out = jnp.dot(hot_hidden, hot_down, preferred_element_type=jnp.float32)
    padded_tokens = jnp.concatenate([tokens, jnp.zeros((1, D), tokens.dtype)], axis=0)
    span = COLD_DEV * BLOCK

    def add_group(running, group_index):
        group_bits = lax.dynamic_slice_in_dim(cold_bits, (group_index * COLD_DEV).astype(jnp.int32), COLD_DEV, 1)
        group_hit = jnp.max(group_bits, axis=1) > 0
        picked = jnp.nonzero(group_hit, size=N_COLD * CAP, fill_value=TOKENS)[0].astype(jnp.int32)
        padded_bits = jnp.concatenate([group_bits, jnp.zeros((1, COLD_DEV), group_bits.dtype)], axis=0)
        picked_rows = jnp.take(padded_tokens, picked, axis=0)
        picked_bits = jnp.take(padded_bits, picked, axis=0)
        first_col = (group_index * span).astype(jnp.int32)
        gate_part = lax.dynamic_slice_in_dim(cold_gate, first_col, span, 1)
        up_part = lax.dynamic_slice_in_dim(cold_up, first_col, span, 1)
        down_part = lax.dynamic_slice_in_dim(cold_down, first_col, span, 0)
        gate_sum = ranged_product(picked_rows, gate_part)
        up_sum = ranged_product(picked_rows, up_part)
        scale = jnp.repeat(picked_bits.astype(jnp.float32), BLOCK, axis=1)
        hidden = (jax.nn.silu(gate_sum) * up_sum * scale).astype(jnp.bfloat16)
        group_out = jnp.dot(hidden, down_part, preferred_element_type=jnp.float32)
        return running.at[picked].add(group_out), None

    initial = jnp.zeros((TOKENS + 1, D), jnp.float32)
    cold_out = lax.scan(add_group, initial, jnp.arange(N_COLD, dtype=jnp.int32))[0]
    return (hot_out + cold_out[:TOKENS]).astype(jnp.bfloat16)
```

```python
import functools

import jax
import jax.numpy as jnp
from jax import lax
from jax.experimental import pallas as pl
from jax.experimental.pallas import tpu as pltpu
from jax.sharding import PartitionSpec as P

BLOCK = 128
F32 = jnp.float32
BF16 = jnp.bfloat16
VM = pl.BlockSpec(memory_space=pltpu.VMEM)
SM = pl.BlockSpec(memory_space=pltpu.SMEM)
HB = pl.BlockSpec(memory_space=pl.ANY)


def params(mib):
    return pltpu.CompilerParams(vmem_limit_bytes=mib * 1024 * 1024)


def send(value, axis, size, mask):
    return lax.ppermute(value, axis, [(at, at ^ mask) for at in range(size)])


def route_kernel(place, ids, mask, pick, spread, row_bits, bits, ordered, *, order, rows, cold_blocks, hot_blocks):
    total, named = mask.shape
    own = place[0]
    groups = len(order)
    for at, mark in enumerate(order):
        first = pl.multiple_of((own ^ mark) * rows, rows)
        ordered[at * rows : (at + 1) * rows, :] = mask[pl.ds(first, rows), :]
    width = bits.shape[1]
    wanted = jnp.full((width, named), -1, jnp.int32)
    row = lax.broadcasted_iota(jnp.int32, (width, named), 0)
    for at in range(cold_blocks):
        wanted = jnp.where(row == at, ids[own * cold_blocks + at], wanted)
    for at in range(hot_blocks):
        hot_at = groups * cold_blocks + own * hot_blocks + at
        wanted = jnp.where(row == cold_blocks + at, ids[hot_at], wanted)
    column = lax.broadcasted_iota(jnp.int32, (width, named), 1)
    choose = (wanted == column).astype(F32).astype(BF16)
    active = ordered[...].astype(F32).astype(BF16)
    contract = (((1,), (1,)), ((), ()))
    by_token = lax.dot_general(active, choose, contract, preferred_element_type=F32)
    by_block = lax.dot_general(choose, active, contract, preferred_element_type=F32)
    bits[...] = by_token
    lane = lax.broadcasted_iota(jnp.int32, by_token.shape, 1)
    hit_col = jnp.max(jnp.where(lane < cold_blocks, by_token, 0.0), axis=1, keepdims=True)
    line = lax.broadcasted_iota(jnp.int32, by_block.shape, 0)
    hit_row = jnp.max(jnp.where(line < cold_blocks, by_block, 0.0), axis=0, keepdims=True)
    down = lax.broadcasted_iota(jnp.int32, (total, total), 0)
    across = lax.broadcasted_iota(jnp.int32, (total, total), 1)
    rank_col = jnp.sum(jnp.where(across < down, hit_row, 0.0), axis=1, keepdims=True)
    rank_row = jnp.sum(jnp.where(down < across, hit_col, 0.0), axis=0, keepdims=True)
    slot_row = jnp.where(hit_row > 0.0, rank_row, -1.0)
    slot_col = jnp.where(hit_col > 0.0, rank_col, -1.0)
    slots = total // 2
    chosen = lax.broadcasted_iota(jnp.int32, (slots, total), 0).astype(F32) == slot_row
    chosen = chosen.astype(F32).astype(BF16)
    pick[...] = chosen
    back = lax.broadcasted_iota(jnp.int32, (total, slots), 1).astype(F32) == slot_col
    spread[...] = back.astype(F32).astype(BF16)
    row_bits[...] = jnp.dot(chosen, by_token.astype(BF16), preferred_element_type=F32)


def chunk_of(width):
    return 256 if width % 256 == 0 else 128


def up_kernel(place, near, far, pick, hot_gate, hot_up, cold_gate, cold_up, *rest, parts):
    outs = rest[:parts]
    hot_gate_v, hot_up_v, cold_gate_v, cold_up_v, sums, sems = rest[parts:]
    cold_width = cold_gate.shape[1]
    hot_width = hot_gate.shape[1]
    step = chunk_of(cold_width)
    half = near.shape[0]
    gates = cold_width + 2 * hot_width
    moves = []
    for source, target in ((cold_gate, cold_gate_v), (cold_up, cold_up_v)):
        for at in range(0, cold_width, step):
            piece = pl.ds(at, step)
            moves.append((source.at[:, piece], target.at[:, piece]))
    moves.append((hot_gate, hot_gate_v))
    moves.append((hot_up, hot_up_v))
    copies = [pltpu.make_async_copy(a, b, sems.at[n]) for n, (a, b) in enumerate(moves)]
    for copy in copies:
        copy.start()
    near_rows = near[...]
    far_rows = far[...]
    picked = jnp.dot(pick[:, :half], near_rows, preferred_element_type=F32)
    picked = picked + jnp.dot(pick[:, half:], far_rows, preferred_element_type=F32)
    picked = picked.astype(BF16)
    at_copy = 0
    for base, target in ((0, cold_gate_v), (gates, cold_up_v)):
        for at in range(0, cold_width, step):
            copies[at_copy].wait()
            at_copy += 1
            value = jnp.dot(picked, target[:, at : at + step], preferred_element_type=F32)
            sums[:, base + at : base + at + step] = value.astype(BF16)
    for base, target in ((0, hot_gate_v), (gates, hot_up_v)):
        copies[at_copy].wait()
        at_copy += 1
        for side, rows in enumerate((near_rows, far_rows)):
            at = base + cold_width + side * hot_width
            value = jnp.dot(rows, target[...], preferred_element_type=F32)
            sums[:, at : at + hot_width] = value.astype(BF16)
    share = half // parts
    for mark, out in enumerate(outs):
        first = pl.multiple_of((place[1] ^ mark) * share, share)
        out[...] = sums[pl.ds(first, share), :]


def act_kernel(place, row_bits, bits, *rest, cold_blocks, hot_blocks):
    out = rest[-1]
    terms = rest[:-1]
    share = out.shape[0]
    gates = out.shape[1]
    slots = row_bits.shape[0]
    total = terms[0][...].astype(F32)
    for term in terms[1:]:
        total = total + term[...].astype(F32)
    first = pl.multiple_of(place[1] * share, share)
    cold_rows = row_bits[pl.ds(first, share), :]
    columns = [cold_rows[:, at : at + 1] for at in range(cold_blocks)]
    for side in range(2):
        begin = pl.multiple_of(side * slots + place[1] * share, share)
        hot_rows = bits[pl.ds(begin, share), :]
        columns += [hot_rows[:, cold_blocks + at : cold_blocks + at + 1] for at in range(hot_blocks)]
    for at, column in enumerate(columns):
        gate = total[:, at * BLOCK : (at + 1) * BLOCK]
        up = total[:, gates + at * BLOCK : gates + (at + 1) * BLOCK]
        value = gate / (1.0 + jnp.exp(-gate)) * up * column
        out[:, at * BLOCK : (at + 1) * BLOCK] = value.astype(BF16)


def down_kernel(place, spread, cold_down, hot_down, *rest, parts):
    blocks = rest[:parts]
    near, far, cold_v, hot_v, hidden, sems = rest[parts:]
    cold_width, features = cold_down.shape
    hot_width = hot_down.shape[0]
    step = chunk_of(features)
    copies = []
    for at in range(0, features, step):
        piece = pl.ds(at, step)
        slot = at // step
        copies.append(pltpu.make_async_copy(cold_down.at[:, piece], cold_v.at[:, piece], sems.at[0, slot]))
        copies.append(pltpu.make_async_copy(hot_down.at[:, piece], hot_v.at[:, piece], sems.at[1, slot]))
    for copy in copies:
        copy.start()
    share = blocks[0].shape[0]
    for mark, block in enumerate(blocks):
        first = pl.multiple_of((place[1] ^ mark) * share, share)
        hidden[pl.ds(first, share), :] = block[...]
    half = near.shape[0]
    cold_rows = jnp.dot(spread[...], hidden[:, :cold_width], preferred_element_type=F32).astype(BF16)
    hot_near = hidden[:, cold_width : cold_width + hot_width]
    hot_far = hidden[:, cold_width + hot_width :]
    hot_rows = jnp.concatenate([hot_near, hot_far], axis=0)
    for at in range(0, features, step):
        copies[2 * (at // step)].wait()
        copies[2 * (at // step) + 1].wait()
        value = jnp.dot(cold_rows, cold_v[:, at : at + step], preferred_element_type=F32)
        value = value + jnp.dot(hot_rows, hot_v[:, at : at + step], preferred_element_type=F32)
        value = value.astype(BF16)
        near[:, at : at + step] = value[:half]
        far[:, at : at + step] = value[half:]


def body(
    tokens, hot_gate, hot_up, hot_down, cold_gate, cold_up, cold_down, hot_ids, cold_ids, block_mask
):
    groups = lax.axis_size("cold")
    ranges = lax.axis_size("hot")
    place = jnp.stack([lax.axis_index("cold"), lax.axis_index("hot")]).astype(jnp.int32)
    rows, features = tokens.shape
    total, named = block_mask.shape
    half = total // 2
    share = half // ranges
    hot_width = hot_gate.shape[1]
    cold_width = cold_gate.shape[1]
    hot_blocks = hot_width // BLOCK
    cold_blocks = cold_width // BLOCK
    gates = cold_width + 2 * hot_width
    order = list(range(0, groups, 2)) + list(range(1, groups, 2))
    bits_width = -(-(cold_blocks + hot_blocks) // 8) * 8

    near = [tokens] + [send(tokens, "cold", groups, mark) for mark in range(2, groups, 2)]
    near = jnp.concatenate(near, axis=0)
    far = send(near, "cold", groups, 1)

    ids = jnp.concatenate([cold_ids, hot_ids])
    pick, spread, row_bits, bits = pl.pallas_call(
        functools.partial(
            route_kernel, order=order, rows=rows, cold_blocks=cold_blocks, hot_blocks=hot_blocks
        ),
        out_shape=(
            jax.ShapeDtypeStruct((half, total), BF16),
            jax.ShapeDtypeStruct((total, half), BF16),
            jax.ShapeDtypeStruct((half, bits_width), F32),
            jax.ShapeDtypeStruct((total, bits_width), F32),
        ),
        in_specs=[SM, SM, VM],
        out_specs=(VM, VM, VM, VM),
        scratch_shapes=[pltpu.VMEM((total, named), jnp.int32)],
        compiler_params=params(16),
        name="route",
    )(place, ids, block_mask)

    copies = 2 * (cold_width // chunk_of(cold_width)) + 2
    partial_sums = pl.pallas_call(
        functools.partial(up_kernel, parts=ranges),
        out_shape=tuple(jax.ShapeDtypeStruct((share, 2 * gates), BF16) for _ in range(ranges)),
        in_specs=[SM, VM, VM, VM, HB, HB, HB, HB],
        out_specs=tuple(VM for _ in range(ranges)),
        scratch_shapes=[
            pltpu.VMEM((features, hot_width), BF16),
            pltpu.VMEM((features, hot_width), BF16),
            pltpu.VMEM((features, cold_width), BF16),
            pltpu.VMEM((features, cold_width), BF16),
            pltpu.VMEM((half, 2 * gates), BF16),
            pltpu.SemaphoreType.DMA((copies,)),
        ],
        compiler_params=params(24),
        name="up",
    )(place, near, far, pick, hot_gate, hot_up, cold_gate, cold_up)

    terms = [partial_sums[0]]
    terms += [send(partial_sums[mark], "hot", ranges, mark) for mark in range(1, ranges)]
    own_hidden = pl.pallas_call(
        functools.partial(act_kernel, cold_blocks=cold_blocks, hot_blocks=hot_blocks),
        out_shape=jax.ShapeDtypeStruct((share, gates), BF16),
        in_specs=[SM, VM, VM] + [VM] * ranges,
        out_specs=VM,
        compiler_params=params(16),
        name="act",
    )(place, row_bits, bits, *terms)

    blocks = [own_hidden] + [send(own_hidden, "hot", ranges, mark) for mark in range(1, ranges)]
    near_out, far_out = pl.pallas_call(
        functools.partial(down_kernel, parts=ranges),
        out_shape=(
            jax.ShapeDtypeStruct((half, features), BF16),
            jax.ShapeDtypeStruct((half, features), BF16),
        ),
        in_specs=[SM, VM, HB, HB] + [VM] * ranges,
        out_specs=(VM, VM),
        scratch_shapes=[
            pltpu.VMEM((cold_width, features), BF16),
            pltpu.VMEM((hot_width, features), BF16),
            pltpu.VMEM((half, gates), BF16),
            pltpu.SemaphoreType.DMA((2, features // chunk_of(features))),
        ],
        compiler_params=params(24),
        name="down",
    )(place, spread, cold_down, hot_down, *blocks)

    pair = near_out.astype(F32) + send(far_out, "cold", groups, 1).astype(F32)
    result = pair[:rows]
    for at in range(1, groups // 2):
        piece = pair[at * rows : (at + 1) * rows].astype(BF16)
        result = result + send(piece, "cold", groups, 2 * at).astype(F32)
    return result.astype(BF16)


def solution(mesh):
    return jax.shard_map(
        body,
        mesh=mesh,
        in_specs=(
            P("cold", "hot"),
            P("hot", "cold"),
            P("hot", "cold"),
            P("cold", "hot"),
            P("hot", "cold"),
            P("hot", "cold"),
            P("cold", "hot"),
            P(),
            P(),
            P(),
        ),
        out_specs=P("cold", "hot"),
        check_vma=False,
    )
```

```python
import functools

import jax
import jax.numpy as jnp
from jax import lax
from jax.experimental import pallas as pl
from jax.experimental.pallas import tpu as pltpu
from jax.sharding import PartitionSpec as P

BLOCK = 128
F32 = jnp.float32
BF16 = jnp.bfloat16
WIRE = jnp.bfloat16
VM = pl.BlockSpec(memory_space=pltpu.VMEM)
SM = pl.BlockSpec(memory_space=pltpu.SMEM)
HB = pl.BlockSpec(memory_space=pltpu.HBM)


def cost(flops):
    return pl.CostEstimate(flops=flops, bytes_accessed=0, transcendentals=0)


def params(mib):
    return pltpu.CompilerParams(vmem_limit_bytes=mib * 1024 * 1024)


def send(value, axis, size, mask):
    return lax.ppermute(value, axis, [(at, at ^ mask) for at in range(size)])


def route_kernel(
    cold_at, cold_ids, hot_ids, mask, *rest, order, rows, cold_blocks, hot_blocks, weights
):
    sources = rest[:weights]
    pick, spread, row_bits, bits = rest[weights : weights + 4]
    targets = rest[weights + 4 : 2 * weights + 4]
    ordered, sems = rest[2 * weights + 4 :]
    copies = [
        pltpu.make_async_copy(a, b, sems.at[n]) for n, (a, b) in enumerate(zip(sources, targets))
    ]
    for copy in copies:
        copy.start()
    total, named = mask.shape
    own = cold_at[0]
    for at, mark in enumerate(order):
        first = pl.multiple_of((own ^ mark) * rows, rows)
        ordered[at * rows : (at + 1) * rows, :] = mask[pl.ds(first, rows), :]
    width = bits.shape[1]
    wanted = jnp.full((width, named), -1, jnp.int32)
    row = lax.broadcasted_iota(jnp.int32, (width, named), 0)
    for at in range(cold_blocks):
        wanted = jnp.where(row == at, cold_ids[own * cold_blocks + at], wanted)
    for at in range(hot_blocks):
        wanted = jnp.where(row == cold_blocks + at, hot_ids[own * hot_blocks + at], wanted)
    column = lax.broadcasted_iota(jnp.int32, (width, named), 1)
    choose = (wanted == column).astype(F32).astype(BF16)
    active = ordered[...].astype(F32).astype(BF16)
    contract = (((1,), (1,)), ((), ()))
    by_token = lax.dot_general(active, choose, contract, preferred_element_type=F32)
    by_block = lax.dot_general(choose, active, contract, preferred_element_type=F32)
    bits[...] = by_token
    lane = lax.broadcasted_iota(jnp.int32, by_token.shape, 1)
    hit_col = jnp.max(jnp.where(lane < cold_blocks, by_token, 0.0), axis=1, keepdims=True)
    line = lax.broadcasted_iota(jnp.int32, by_block.shape, 0)
    hit_row = jnp.max(jnp.where(line < cold_blocks, by_block, 0.0), axis=0, keepdims=True)
    down = lax.broadcasted_iota(jnp.int32, (total, total), 0)
    across = lax.broadcasted_iota(jnp.int32, (total, total), 1)
    rank_col = jnp.sum(jnp.where(across < down, hit_row, 0.0), axis=1, keepdims=True)
    rank_row = jnp.sum(jnp.where(down < across, hit_col, 0.0), axis=0, keepdims=True)
    slot_row = jnp.where(hit_row > 0.0, rank_row, -1.0)
    slot_col = jnp.where(hit_col > 0.0, rank_col, -1.0)
    slots = total // 2
    chosen = lax.broadcasted_iota(jnp.int32, (slots, total), 0).astype(F32) == slot_row
    chosen = chosen.astype(F32).astype(BF16)
    pick[...] = chosen
    back = lax.broadcasted_iota(jnp.int32, (total, slots), 1).astype(F32) == slot_col
    spread[...] = back.astype(F32).astype(BF16)
    row_bits[...] = jnp.dot(chosen, by_token.astype(BF16), preferred_element_type=F32)
    for copy in copies:
        copy.wait()


def chunk_of(width):
    return 256 if width % 256 == 0 else 128


def up_kernel(hot_at, near, far, pick, hot_gate, hot_up, cold_gate, cold_up, *rest, parts):
    outs = rest[:parts]
    sums = rest[parts]
    cold_width = cold_gate.shape[1]
    hot_width = hot_gate.shape[1]
    step = chunk_of(cold_width)
    half = near.shape[0]
    gates = cold_width + 2 * hot_width
    near_rows = near[...]
    far_rows = far[...]
    picked = jnp.dot(pick[:, :half], near_rows, preferred_element_type=F32)
    picked = picked + jnp.dot(pick[:, half:], far_rows, preferred_element_type=F32)
    picked = picked.astype(BF16)
    for base, weight in ((0, hot_gate), (gates, hot_up)):
        for side, rows in enumerate((near_rows, far_rows)):
            at = base + cold_width + side * hot_width
            sums[:, at : at + hot_width] = jnp.dot(rows, weight[...], preferred_element_type=F32)
    for base, weight in ((0, cold_gate), (gates, cold_up)):
        for at in range(0, cold_width, step):
            value = jnp.dot(picked, weight[:, at : at + step], preferred_element_type=F32)
            sums[:, base + at : base + at + step] = value
    share = half // parts
    for mark, out in enumerate(outs):
        first = pl.multiple_of((hot_at[0] ^ mark) * share, share)
        out[...] = sums[pl.ds(first, share), :].astype(out.dtype)


def act_kernel(hot_at, row_bits, bits, *rest, cold_blocks, hot_blocks):
    out = rest[-1]
    terms = rest[:-1]
    share = out.shape[0]
    gates = out.shape[1]
    slots = row_bits.shape[0]
    total = terms[0][...].astype(F32)
    for term in terms[1:]:
        total = total + term[...].astype(F32)
    first = pl.multiple_of(hot_at[0] * share, share)
    cold_rows = row_bits[pl.ds(first, share), :]
    columns = [cold_rows[:, at : at + 1] for at in range(cold_blocks)]
    for side in range(2):
        begin = pl.multiple_of(side * slots + hot_at[0] * share, share)
        hot_rows = bits[pl.ds(begin, share), :]
        columns += [hot_rows[:, cold_blocks + at : cold_blocks + at + 1] for at in range(hot_blocks)]
    for at, column in enumerate(columns):
        gate = total[:, at * BLOCK : (at + 1) * BLOCK]
        up = total[:, gates + at * BLOCK : gates + (at + 1) * BLOCK]
        value = gate / (1.0 + jnp.exp(-gate)) * up * column
        out[:, at * BLOCK : (at + 1) * BLOCK] = value.astype(BF16)


def down_kernel(hot_at, spread, cold_down, hot_down, *rest, parts, side):
    blocks = rest[:parts]
    out, hidden = rest[parts:]
    cold_width, features = cold_down.shape
    hot_width = hot_down.shape[0]
    step = chunk_of(features)
    share = blocks[0].shape[0]
    for mark, block in enumerate(blocks):
        first = pl.multiple_of((hot_at[0] ^ mark) * share, share)
        hidden[pl.ds(first, share), :] = block[...]
    half = out.shape[0]
    rows = spread[side * half : (side + 1) * half, :]
    cold_rows = jnp.dot(rows, hidden[:, :cold_width], preferred_element_type=F32).astype(BF16)
    first = cold_width + side * hot_width
    hot_rows = hidden[:, first : first + hot_width]
    for at in range(0, features, step):
        value = jnp.dot(cold_rows, cold_down[:, at : at + step], preferred_element_type=F32)
        value = value + jnp.dot(hot_rows, hot_down[:, at : at + step], preferred_element_type=F32)
        out[:, at : at + step] = value.astype(out.dtype)


def body(
    tokens, hot_gate, hot_up, hot_down, cold_gate, cold_up, cold_down, hot_ids, cold_ids, block_mask
):
    groups = lax.axis_size("cold")
    ranges = lax.axis_size("hot")
    cold_at = lax.axis_index("cold").astype(jnp.int32).reshape(1)
    hot_at = lax.axis_index("hot").astype(jnp.int32).reshape(1)
    rows, features = tokens.shape
    total, named = block_mask.shape
    half = total // 2
    share = half // ranges
    hot_width = hot_gate.shape[1]
    cold_width = cold_gate.shape[1]
    hot_blocks = hot_width // BLOCK
    cold_blocks = cold_width // BLOCK
    gates = cold_width + 2 * hot_width
    order = list(range(0, groups, 2)) + list(range(1, groups, 2))
    bits_width = -(-(cold_blocks + hot_blocks) // 8) * 8

    near = [tokens] + [send(tokens, "cold", groups, mark) for mark in range(2, groups, 2)]
    near = jnp.concatenate(near, axis=0)
    far = send(near, "cold", groups, 1)

    weights = (hot_gate, hot_up, cold_gate, cold_up)
    weights = tuple(pltpu.with_memory_space_constraint(item, pltpu.HBM) for item in weights)
    routed = pl.pallas_call(
        functools.partial(
            route_kernel,
            order=order,
            rows=rows,
            cold_blocks=cold_blocks,
            hot_blocks=hot_blocks,
            weights=len(weights),
        ),
        out_shape=(
            jax.ShapeDtypeStruct((half, total), BF16),
            jax.ShapeDtypeStruct((total, half), BF16),
            jax.ShapeDtypeStruct((half, bits_width), F32),
            jax.ShapeDtypeStruct((total, bits_width), F32),
            *(jax.ShapeDtypeStruct(weight.shape, weight.dtype) for weight in weights),
        ),
        in_specs=[SM, SM, SM, VM] + [HB] * len(weights),
        out_specs=(VM,) * (4 + len(weights)),
        scratch_shapes=[
            pltpu.VMEM((total, named), jnp.int32),
            pltpu.SemaphoreType.DMA((len(weights),)),
        ],
        compiler_params=params(24),
        cost_estimate=cost(50_000_000),
        name="route",
    )(cold_at, cold_ids, hot_ids, block_mask, *weights)
    pick, spread, row_bits, bits = routed[:4]

    partial_sums = pl.pallas_call(
        functools.partial(up_kernel, parts=ranges),
        out_shape=tuple(
            jax.ShapeDtypeStruct((share, 2 * gates), WIRE if mark else F32) for mark in range(ranges)
        ),
        in_specs=[SM, VM, VM, VM, VM, VM, VM, VM],
        out_specs=tuple(VM for _ in range(ranges)),
        scratch_shapes=[pltpu.VMEM((half, 2 * gates), F32)],
        compiler_params=params(24),
        name="up",
    )(hot_at, near, far, pick, *routed[4:])

    terms = [partial_sums[0]]
    terms += [send(partial_sums[mark], "hot", ranges, mark) for mark in range(1, ranges)]
    own_hidden = pl.pallas_call(
        functools.partial(act_kernel, cold_blocks=cold_blocks, hot_blocks=hot_blocks),
        out_shape=jax.ShapeDtypeStruct((share, gates), BF16),
        in_specs=[SM, VM, VM] + [VM] * ranges,
        out_specs=VM,
        compiler_params=params(16),
        name="act",
    )(hot_at, row_bits, bits, *terms)

    blocks = [own_hidden] + [send(own_hidden, "hot", ranges, mark) for mark in range(1, ranges)]

    def down(side, kind):
        return pl.pallas_call(
            functools.partial(down_kernel, parts=ranges, side=side),
            out_shape=jax.ShapeDtypeStruct((half, features), kind),
            in_specs=[SM, VM, VM, VM] + [VM] * ranges,
            out_specs=VM,
            scratch_shapes=[pltpu.VMEM((half, gates), BF16)],
            compiler_params=params(24),
            cost_estimate=cost(20_000_000),
            name=f"down{side}",
        )(hot_at, spread, cold_down, hot_down, *blocks)

    far_back = send(down(1, BF16), "cold", groups, 1)
    pair = down(0, F32) + far_back.astype(F32)
    result = pair[:rows]
    for at in range(1, groups // 2):
        piece = pair[at * rows : (at + 1) * rows].astype(BF16)
        result = result + send(piece, "cold", groups, 2 * at).astype(F32)
    return result.astype(BF16)


def solution(mesh):
    return jax.shard_map(
        body,
        mesh=mesh,
        in_specs=(
            P("cold", "hot"),
            P("hot", "cold"),
            P("hot", "cold"),
            P("cold", "hot"),
            P("hot", "cold"),
            P("hot", "cold"),
            P("cold", "hot"),
            P(),
            P(),
            P(),
        ),
        out_specs=P("cold", "hot"),
        check_vma=False,
    )
```

```python
import functools

import jax
import jax.numpy as jnp
from jax import lax
from jax.experimental import pallas as pl
from jax.experimental.pallas import tpu as pltpu
from jax.sharding import PartitionSpec as P

BLOCK = 128
F32 = jnp.float32
BF16 = jnp.bfloat16
WIRE = jnp.bfloat16
VM = pl.BlockSpec(memory_space=pltpu.VMEM)
SM = pl.BlockSpec(memory_space=pltpu.SMEM)
HB = pl.BlockSpec(memory_space=pltpu.HBM)


def cost(flops):
    return pl.CostEstimate(flops=flops, bytes_accessed=0, transcendentals=0)


def params(mib):
    return pltpu.CompilerParams(vmem_limit_bytes=mib * 1024 * 1024)


def send(value, axis, size, mask):
    return lax.ppermute(value, axis, [(at, at ^ mask) for at in range(size)])


def route_kernel(
    cold_at, cold_ids_in, hot_ids_in, mask_in, *rest, order, rows, cold_blocks, hot_blocks, weights
):
    sources = rest[:weights]
    pick, spread, row_bits, bits = rest[weights : weights + 4]
    targets = rest[weights + 4 : 2 * weights + 4]
    ordered, mask, turned, cold_ids, hot_ids, sems = rest[2 * weights + 4 :]
    tables = ((mask_in, turned), (cold_ids_in, cold_ids), (hot_ids_in, hot_ids))
    early = [
        pltpu.make_async_copy(a, b, sems.at[weights + n]) for n, (a, b) in enumerate(tables)
    ]
    for copy in early:
        copy.start()
    copies = [
        pltpu.make_async_copy(a, b, sems.at[n]) for n, (a, b) in enumerate(zip(sources, targets))
    ]
    for copy in copies:
        copy.start()
    for copy in early:
        copy.wait()
    mask[...] = turned[...].T
    total, named = mask.shape
    own = cold_at[0]
    for at, mark in enumerate(order):
        first = pl.multiple_of((own ^ mark) * rows, rows)
        ordered[at * rows : (at + 1) * rows, :] = mask[pl.ds(first, rows), :]
    width = bits.shape[1]
    wanted = jnp.full((width, named), -1, jnp.int32)
    row = lax.broadcasted_iota(jnp.int32, (width, named), 0)
    for at in range(cold_blocks):
        wanted = jnp.where(row == at, cold_ids[own * cold_blocks + at], wanted)
    for at in range(hot_blocks):
        wanted = jnp.where(row == cold_blocks + at, hot_ids[own * hot_blocks + at], wanted)
    column = lax.broadcasted_iota(jnp.int32, (width, named), 1)
    choose = (wanted == column).astype(F32).astype(BF16)
    active = ordered[...].astype(F32).astype(BF16)
    contract = (((1,), (1,)), ((), ()))
    by_token = lax.dot_general(active, choose, contract, preferred_element_type=F32)
    by_block = lax.dot_general(choose, active, contract, preferred_element_type=F32)
    bits[...] = by_token
    lane = lax.broadcasted_iota(jnp.int32, by_token.shape, 1)
    hit_col = jnp.max(jnp.where(lane < cold_blocks, by_token, 0.0), axis=1, keepdims=True)
    line = lax.broadcasted_iota(jnp.int32, by_block.shape, 0)
    hit_row = jnp.max(jnp.where(line < cold_blocks, by_block, 0.0), axis=0, keepdims=True)
    down = lax.broadcasted_iota(jnp.int32, (total, total), 0)
    across = lax.broadcasted_iota(jnp.int32, (total, total), 1)
    rank_col = jnp.sum(jnp.where(across < down, hit_row, 0.0), axis=1, keepdims=True)
    rank_row = jnp.sum(jnp.where(down < across, hit_col, 0.0), axis=0, keepdims=True)
    slot_row = jnp.where(hit_row > 0.0, rank_row, -1.0)
    slot_col = jnp.where(hit_col > 0.0, rank_col, -1.0)
    slots = total // 2
    chosen = lax.broadcasted_iota(jnp.int32, (slots, total), 0).astype(F32) == slot_row
    chosen = chosen.astype(F32).astype(BF16)
    pick[...] = chosen
    back = lax.broadcasted_iota(jnp.int32, (total, slots), 1).astype(F32) == slot_col
    spread[...] = back.astype(F32).astype(BF16)
    row_bits[...] = jnp.dot(chosen, by_token.astype(BF16), preferred_element_type=F32)
    for copy in copies:
        copy.wait()


def chunk_of(width):
    return 256 if width % 256 == 0 else 128


def up_kernel(hot_at, near, far, pick, hot_gate, hot_up, cold_gate, cold_up, *rest, parts):
    outs = rest[:parts]
    sums = rest[parts]
    cold_width = cold_gate.shape[1]
    hot_width = hot_gate.shape[1]
    step = chunk_of(cold_width)
    half = near.shape[0]
    gates = cold_width + 2 * hot_width
    near_rows = near[...]
    far_rows = far[...]
    picked = jnp.dot(pick[:, :half], near_rows, preferred_element_type=F32)
    picked = picked + jnp.dot(pick[:, half:], far_rows, preferred_element_type=F32)
    picked = picked.astype(BF16)
    for base, weight in ((0, hot_gate), (gates, hot_up)):
        for side, rows in enumerate((near_rows, far_rows)):
            at = base + cold_width + side * hot_width
            sums[:, at : at + hot_width] = jnp.dot(rows, weight[...], preferred_element_type=F32)
    for base, weight in ((0, cold_gate), (gates, cold_up)):
        for at in range(0, cold_width, step):
            value = jnp.dot(picked, weight[:, at : at + step], preferred_element_type=F32)
            sums[:, base + at : base + at + step] = value
    share = half // parts
    for mark, out in enumerate(outs):
        first = pl.multiple_of((hot_at[0] ^ mark) * share, share)
        out[...] = sums[pl.ds(first, share), :].astype(out.dtype)


def act_kernel(hot_at, row_bits, bits, *rest, cold_blocks, hot_blocks):
    out = rest[-1]
    terms = rest[:-1]
    share = out.shape[0]
    gates = out.shape[1]
    slots = row_bits.shape[0]
    total = terms[0][...].astype(F32)
    for term in terms[1:]:
        total = total + term[...].astype(F32)
    first = pl.multiple_of(hot_at[0] * share, share)
    cold_rows = row_bits[pl.ds(first, share), :]
    columns = [cold_rows[:, at : at + 1] for at in range(cold_blocks)]
    for side in range(2):
        begin = pl.multiple_of(side * slots + hot_at[0] * share, share)
        hot_rows = bits[pl.ds(begin, share), :]
        columns += [hot_rows[:, cold_blocks + at : cold_blocks + at + 1] for at in range(hot_blocks)]
    for at, column in enumerate(columns):
        gate = total[:, at * BLOCK : (at + 1) * BLOCK]
        up = total[:, gates + at * BLOCK : gates + (at + 1) * BLOCK]
        value = gate / (1.0 + jnp.exp(-gate)) * up * column
        out[:, at * BLOCK : (at + 1) * BLOCK] = value.astype(BF16)


def down_kernel(hot_at, spread, cold_down, hot_down, *rest, parts, side):
    blocks = rest[:parts]
    out, hidden = rest[parts:]
    cold_width, features = cold_down.shape
    hot_width = hot_down.shape[0]
    step = chunk_of(features)
    share = blocks[0].shape[0]
    for mark, block in enumerate(blocks):
        first = pl.multiple_of((hot_at[0] ^ mark) * share, share)
        hidden[pl.ds(first, share), :] = block[...]
    half = out.shape[0]
    rows = spread[side * half : (side + 1) * half, :]
    cold_rows = jnp.dot(rows, hidden[:, :cold_width], preferred_element_type=F32).astype(BF16)
    first = cold_width + side * hot_width
    hot_rows = hidden[:, first : first + hot_width]
    for at in range(0, features, step):
        value = jnp.dot(cold_rows, cold_down[:, at : at + step], preferred_element_type=F32)
        value = value + jnp.dot(hot_rows, hot_down[:, at : at + step], preferred_element_type=F32)
        out[:, at : at + step] = value.astype(out.dtype)


def body(
    tokens, hot_gate, hot_up, hot_down, cold_gate, cold_up, cold_down, hot_ids, cold_ids, block_mask
):
    groups = lax.axis_size("cold")
    ranges = lax.axis_size("hot")
    cold_at = lax.axis_index("cold").astype(jnp.int32).reshape(1)
    hot_at = lax.axis_index("hot").astype(jnp.int32).reshape(1)
    rows, features = tokens.shape
    total, named = block_mask.shape
    half = total // 2
    share = half // ranges
    hot_width = hot_gate.shape[1]
    cold_width = cold_gate.shape[1]
    hot_blocks = hot_width // BLOCK
    cold_blocks = cold_width // BLOCK
    gates = cold_width + 2 * hot_width
    order = list(range(0, groups, 2)) + list(range(1, groups, 2))
    bits_width = -(-(cold_blocks + hot_blocks) // 8) * 8

    near = [tokens] + [send(tokens, "cold", groups, mark) for mark in range(2, groups, 2)]
    near = jnp.concatenate(near, axis=0)
    far = send(near, "cold", groups, 1)

    weights = (hot_gate, hot_up, cold_gate, cold_up)
    weights = tuple(pltpu.with_memory_space_constraint(item, pltpu.HBM) for item in weights)
    tables = (cold_ids, hot_ids, block_mask.T)
    tables = tuple(pltpu.with_memory_space_constraint(item, pltpu.HBM) for item in tables)
    routed = pl.pallas_call(
        functools.partial(
            route_kernel,
            order=order,
            rows=rows,
            cold_blocks=cold_blocks,
            hot_blocks=hot_blocks,
            weights=len(weights),
        ),
        out_shape=(
            jax.ShapeDtypeStruct((half, total), BF16),
            jax.ShapeDtypeStruct((total, half), BF16),
            jax.ShapeDtypeStruct((half, bits_width), F32),
            jax.ShapeDtypeStruct((total, bits_width), F32),
            *(jax.ShapeDtypeStruct(weight.shape, weight.dtype) for weight in weights),
        ),
        in_specs=[SM, HB, HB, HB] + [HB] * len(weights),
        out_specs=(VM,) * (4 + len(weights)),
        scratch_shapes=[
            pltpu.VMEM((total, named), jnp.int32),
            pltpu.VMEM((total, named), jnp.int32),
            pltpu.VMEM((named, total), jnp.int32),
            pltpu.SMEM(cold_ids.shape, jnp.int32),
            pltpu.SMEM(hot_ids.shape, jnp.int32),
            pltpu.SemaphoreType.DMA((len(weights) + 3,)),
        ],
        compiler_params=params(24),
        cost_estimate=cost(50_000_000),
        name="route",
    )(cold_at, *tables, *weights)
    pick, spread, row_bits, bits = routed[:4]

    partial_sums = pl.pallas_call(
        functools.partial(up_kernel, parts=ranges),
        out_shape=tuple(
            jax.ShapeDtypeStruct((share, 2 * gates), WIRE if mark else F32) for mark in range(ranges)
        ),
        in_specs=[SM, VM, VM, VM, VM, VM, VM, VM],
        out_specs=tuple(VM for _ in range(ranges)),
        scratch_shapes=[pltpu.VMEM((half, 2 * gates), F32)],
        compiler_params=params(24),
        name="up",
    )(hot_at, near, far, pick, *routed[4:])

    terms = [partial_sums[0]]
    terms += [send(partial_sums[mark], "hot", ranges, mark) for mark in range(1, ranges)]
    own_hidden = pl.pallas_call(
        functools.partial(act_kernel, cold_blocks=cold_blocks, hot_blocks=hot_blocks),
        out_shape=jax.ShapeDtypeStruct((share, gates), BF16),
        in_specs=[SM, VM, VM] + [VM] * ranges,
        out_specs=VM,
        compiler_params=params(16),
        name="act",
    )(hot_at, row_bits, bits, *terms)

    blocks = [own_hidden] + [send(own_hidden, "hot", ranges, mark) for mark in range(1, ranges)]

    def down(side, kind):
        return pl.pallas_call(
            functools.partial(down_kernel, parts=ranges, side=side),
            out_shape=jax.ShapeDtypeStruct((half, features), kind),
            in_specs=[SM, VM, VM, VM] + [VM] * ranges,
            out_specs=VM,
            scratch_shapes=[pltpu.VMEM((half, gates), BF16)],
            compiler_params=params(24),
            cost_estimate=cost(20_000_000),
            name=f"down{side}",
        )(hot_at, spread, cold_down, hot_down, *blocks)

    far_back = send(down(1, BF16), "cold", groups, 1)
    pair = down(0, F32) + far_back.astype(F32)
    result = pair[:rows]
    for at in range(1, groups // 2):
        piece = pair[at * rows : (at + 1) * rows].astype(BF16)
        result = result + send(piece, "cold", groups, 2 * at).astype(F32)
    return result.astype(BF16)


def solution(mesh):
    return jax.shard_map(
        body,
        mesh=mesh,
        in_specs=(
            P("cold", "hot"),
            P("hot", "cold"),
            P("hot", "cold"),
            P("cold", "hot"),
            P("hot", "cold"),
            P("hot", "cold"),
            P("cold", "hot"),
            P(),
            P(),
            P(),
        ),
        out_specs=P("cold", "hot"),
        check_vma=False,
    )
```
